16 devices in a mesh: rep: 1, r: 2 (over z), s: 8 (over x, y, core).
Axes of the slice: x: 2, y: 2, z: 2, core: 2. Of those that a mesh axis runs over, the one named last changes fastest.
Arguments:
- x: bfloat16 [16, 2048, 1024], P(('rep', 'r', 's'))
- dy: bfloat16 [16, 2048, 1024], P(('rep', 'r', 's'))
- w_gate: bfloat16 [2, 1024, 4096], P(None, 's')
- w_up: bfloat16 [2, 1024, 4096], P(None, 's')
- w_down: bfloat16 [2, 4096, 1024], P(None, 's')
Outputs:
- output 1: bfloat16 [16, 2048, 1024], P(('rep', 'r', 's'))
- output 2: bfloat16 [2, 1024, 4096], P('rep', 's')
- output 3: bfloat16 [2, 1024, 4096], P('rep', 's')
- output 4: bfloat16 [2, 4096, 1024], P('rep', 's')
All inputs are finite; a program needn't handle non-finite values.
Results may differ from the reference program's by a relative error of at most 0.018.
Values are sent between devices in bfloat16 or wider.
A program may use at most 2 GiB of HBM per device.

```python
import jax
import jax.numpy as jnp
from jax import lax

SEQUENCES = 16
TOKENS = 2048
D = 1024
FF = 4096
LAYERS = 2
NAMES = ("w_gate", "w_up", "w_down")
SHAPES = {"w_gate": (LAYERS, D, FF), "w_up": (LAYERS, D, FF), "w_down": (LAYERS, FF, D)}


def bump(key, n, height):
    away = (jnp.arange(n, dtype=jnp.int32) - jax.random.randint(key, (), 0, n, jnp.int32)) % n
    return jnp.where(away < n // 8, height, 1.0)


def together(key, own, strength):
    shared = jax.random.normal(key, own.shape[1:], jnp.float32)
    return (own + strength * shared) * lax.rsqrt(1 + strength * strength)


def setup_inputs(seed: int = 0, part: int = 0) -> dict:
    kx, kdy, ka, kb, kz, kf, kh, kl, *kw = jax.random.split(jax.random.key(seed), 8 + len(NAMES))
    kx, kdy, ka, kb = (jax.random.fold_in(k, part) for k in (kx, kdy, ka, kb))
    shape = (SEQUENCES, TOKENS, D)
    much_x, much_dy = jax.random.uniform(kz, (2,), jnp.float32, 0.0, 1.0)
    layers = 2.0 ** jax.random.uniform(kl, (LAYERS, 1, 1), jnp.float32, -1.0, 1.0)
    x = together(ka, jax.random.normal(kx, shape, jnp.float32), much_x) * bump(kf, D, 4.0)
    dy = together(kb, jax.random.normal(kdy, shape, jnp.float32), much_dy)
    drawn = {"x": x.astype(jnp.bfloat16), "dy": (dy * (SEQUENCES * TOKENS) ** -0.5).astype(jnp.bfloat16)}
    for key, name in zip(kw, NAMES, strict=True):
        w = jax.random.normal(key, SHAPES[name], jnp.float32) * SHAPES[name][1] ** -0.5
        drawn[name] = (w * {"w_gate": 1.0, "w_up": bump(kh, FF, 4.0), "w_down": layers}[name]).astype(jnp.bfloat16)
    return drawn


def matmul(a, w):
    return jnp.dot(a, w, preferred_element_type=jnp.float32).astype(jnp.bfloat16)


def normed(h):
    wide = h.astype(jnp.float32)
    scale = lax.rsqrt(jnp.mean(wide**2, -1, keepdims=True) + 1e-6)
    return (wide * scale).astype(jnp.bfloat16)


def layer(h, w):
    a = normed(h)
    gate = jnp.dot(a, w["w_gate"], preferred_element_type=jnp.float32)
    up = jnp.dot(a, w["w_up"], preferred_element_type=jnp.float32)
    return h + matmul((jax.nn.silu(gate) * up).astype(jnp.bfloat16), w["w_down"])


def stack(weights, h):
    return lax.scan(lambda h, w: (layer(h, w), None), h, weights)[0]


def reference(x, dy, w_gate, w_up, w_down):
    weights = dict(zip(NAMES, (w_gate, w_up, w_down), strict=True))

    def take(so_far, sequence):
        h, by_y = sequence
        _, back = jax.vjp(stack, weights, h)
        by_weights, by_h = back(by_y)
        return jax.tree.map(lambda total, term: total + term.astype(jnp.float32), so_far, by_weights), by_h

    none_yet = {name: jnp.zeros(w.shape, jnp.float32) for name, w in weights.items()}
    by_weights, by_x = lax.scan(take, none_yet, (x, dy))
    return (by_x, *(by_weights[name].astype(jnp.bfloat16) for name in NAMES))
```

```python
import functools

import jax
import jax.numpy as jnp
from jax import lax
from jax.experimental import pallas as pl
from jax.experimental.pallas import tpu as pltpu
from jax.sharding import PartitionSpec as P

BF, F32 = jnp.bfloat16, jnp.float32
T, D, FF = 2048, 1024, 4096
TN, TM, MC = 512, 256, 1024
VMEM_LIMIT = 67043328
MESH = pl.DeviceIdType.MESH
DMA = pltpu.SemaphoreType.DMA
ANY = pl.BlockSpec(memory_space=pl.ANY)


def sds(shape, dtype=BF):
    return jax.ShapeDtypeStruct(shape, dtype)


def resident(shape):
    return pl.BlockSpec(shape, lambda i: (0, 0), pipeline_mode=pl.Buffered(1))


def columns(rows, cols):
    return pl.BlockSpec((rows, cols), lambda i: (0, i))


def rows_of(rows, cols):
    return pl.BlockSpec((rows, cols), lambda i: (i, 0))


def dot(a, b, ca=1, cb=0):
    return lax.dot_general(a, b, (((ca,), (cb,)), ((), ())), preferred_element_type=F32)


def chunks(total, size, f):
    def go(i, c):
        f(pl.ds(pl.multiple_of(i * size, size), size))
        return c

    lax.fori_loop(0, total // size, go, 0)


class Place:
    def __init__(self):
        self.rep, self.r, self.s = lax.axis_index("rep"), lax.axis_index("r"), lax.axis_index("s")
        s = self.s
        x, y, c = s // 4, (s // 2) % 2, s % 2
        at = lambda x, y, c: x * 4 + y * 2 + c
        self.sx, self.sy, self.sd, self.sc = at(1 - x, y, c), at(x, 1 - y, c), at(1 - x, 1 - y, c), at(x, y, 1 - c)
        self.order = [self.sd, self.sx, self.sy, s]
        self.across = [at(1 - x, 1 - y, 1 - c), at(1 - x, y, 1 - c), at(x, 1 - y, 1 - c), self.sc]
        self.dev = {
            "x": (self.rep, self.r, self.sx),
            "y": (self.rep, self.r, self.sy),
            "z": (self.rep, 1 - self.r, s),
            "c": (self.rep, self.r, self.sc),
        }

    def meet(self):
        barrier = pltpu.get_barrier_semaphore()
        for d in "xyzc":
            pl.semaphore_signal(barrier, inc=1, device_id=self.dev[d], device_id_type=MESH)
        pl.semaphore_wait(barrier, 4)


def rows_at(start, size, unit):
    return pl.ds(pl.multiple_of(start, unit), size)


class Gather:
    TAGS = 17

    def __init__(self, shards, layers, steps):
        self.ins, self.layers, self.steps, n = list(shards), layers, steps, len(shards)
        self.n = n
        self.outs = [sds((8 * a.shape[1], a.shape[2])) for a in shards]
        self.scratch = [pltpu.VMEM(a.shape[1:], BF) for a in shards]
        self.scratch += [DMA((n, 2)), DMA((n, self.TAGS)), DMA((n, self.TAGS))]

    def hooks(self, place, ins, outs, scratch):
        own, (local, send, recv) = scratch[: self.n], scratch[self.n :]
        p = place

        def moves(i):
            shard, whole, layer = ins[i], outs[i], self.layers[i]
            rows = shard.shape[1]
            n = rows // 4
            q = [k + p.r * (3 - 2 * k) for k in range(4)]
            slot = lambda owner, k: whole.at[rows_at(owner * rows + q[k] * n, n, n)]
            three = lambda owner: whole.at[rows_at(owner * rows + p.r * n, 3 * n, n)]
            direct = shard.at[layer, rows_at(p.r * n, 3 * n, n)]
            mine = whole.at[rows_at(p.s * rows, rows, rows)]
            todo = [(direct, three(p.s), "x"), (direct, three(p.s), "y")]
            relay = [(slot(p.sy, 0), "x"), (slot(p.sx, 1), "y"), (slot(p.sx, 0), "z"), (slot(p.sy, 0), "z")]
            relay += [(slot(p.sd, 0), "z"), (slot(p.sd, 1), "z")]
            todo += [(a, a, d) for a, d in relay]
            todo += [(shard.at[layer], mine, "c")]
            core = [three(p.sx), three(p.sy), slot(p.sd, 0), slot(p.sd, 1)]
            core += [slot(p.sx, 3), slot(p.sy, 3), slot(p.sd, 3), slot(p.sd, 2)]
            todo += [(a, a, "c") for a in core]
            def move(t):
                a, b, d = todo[t]
                return pltpu.make_async_remote_copy(a, b, send.at[i, t], recv.at[i, t], device_id=p.dev[d], device_id_type=MESH)

            load = lambda: pltpu.make_async_copy(shard.at[layer], own[i], local.at[i, 0])
            save = lambda: pltpu.make_async_copy(own[i], mine, local.at[i, 1])
            return move, load, save

        def a0(i):
            m, load, _ = moves(i)
            for t in (0, 1, 8):
                m(t).start()
            load().start()

        def a1(i):
            m, load, save = moves(i)
            m(0).wait_recv()
            m(3).start()
            m(4).start()
            m(1).wait_recv()
            for t in (2, 5, 9, 10):
                m(t).start()
            load().wait()
            save().start()

        def a2(i):
            m, _, _ = moves(i)
            m(2).wait_recv()
            m(6).start()
            m(11).start()
            m(3).wait_recv()
            m(7).start()
            m(12).start()

        def a3(i):
            m, _, _ = moves(i)
            for t, u in ((4, 13), (5, 14), (6, 15), (7, 16)):
                m(t).wait_recv()
                m(u).start()

        def a4(i):
            m, _, save = moves(i)
            for t in range(8, 17):
                m(t).wait_recv()
            for t in range(17):
                m(t).wait_send()
            save().wait()

        stage = [a0, a1, a2, a3, a4]
        return [(at, functools.partial(stage[k], i)) for at, k, i in self.steps]


def gather_steps(n, at):
    out = [(at(0), 0, i) for i in range(min(2, n))]
    for k in range(n + 3):
        if 0 <= k < n:
            out.append((at(k + 1), 1, k))
            if k + 2 < n:
                out.append((at(k + 1), 0, k + 2))
        if 0 <= k - 1 < n:
            out.append((at(k + 1), 2, k - 1))
        if 0 <= k - 2 < n:
            out.append((at(k + 1), 3, k - 2))
        if 0 <= k - 3 < n:
            out.append((at(k + 1), 4, k - 3))
    return out


def added(out, *terms):
    rows, cols = out.shape
    size = 65536 // cols

    def one(m):
        total = terms[0][m, :].astype(F32)
        for t in terms[1:]:
            total += t[m, :].astype(F32)
        out[m, :] = total.astype(BF)

    chunks(rows, size, one)


class Scatter:
    def __init__(self, term, at, finish=False):
        self.rows, self.cols = term.shape[0] // 8, term.shape[1]
        self.ins, self.at, self.finish = [term], at, finish
        self.outs = [sds((self.rows, self.cols))]
        block, half = (self.rows, self.cols), (self.rows // 2, self.cols)
        self.scratch = [pltpu.VMEM((4, *block), BF), pltpu.VMEM((4, *block), BF), pltpu.VMEM((2, *half), BF), pltpu.VMEM((2, *block), BF)]
        self.scratch += [DMA((5,)), DMA((11,)), DMA((11,))]
        if finish:
            self.scratch.append(pltpu.VMEM(block, BF))

    def hooks(self, place, ins, outs, scratch):
        p, (term,), (result,) = place, ins, outs
        own, other, diag, side, local, send, recv = scratch[:7]
        rows, h = self.rows, self.rows // 2
        block = lambda b: term.at[rows_at(b * rows, rows, rows)]
        part = lambda ref, k, j: ref.at[k, pl.ds(j * h, h)]

        def move(t, a, b, d):
            return pltpu.make_async_remote_copy(a, b, send.at[t], recv.at[t], device_id=p.dev[d], device_id_type=MESH)

        swap = lambda k: move(k, block(p.across[k]), other.at[k], "c")
        load = lambda k: pltpu.make_async_copy(block(p.order[k]), own.at[k], local.at[k])
        corner = lambda j: move(4 + j, part(other, 0, j), diag.at[j], "xy"[j])
        edge = lambda k, j: move(6 + 2 * k + j, part(other, 1 + k, j), part(side, k, j), "xy"[k])

        def r0():
            for k in range(4):
                swap(k).start()
                load(k).start()

        def ready(k):
            swap(k).wait_recv()
            load(k).wait()

        def r1():
            ready(0)
            for j in range(2):
                added(part(other, 0, j), part(other, 0, j), part(own, 0, j))
                corner(j).start()

        def r2():
            for k in range(2):
                ready(1 + k)
                added(part(other, 1 + k, k), part(other, 1 + k, k), part(own, 1 + k, k))
                edge(k, k).start()

        def r3():
            for k in range(2):
                j = 1 - k
                corner(j).wait_recv()
                added(part(other, 1 + k, j), part(other, 1 + k, j), part(own, 1 + k, j), diag.at[j])
                edge(k, j).start()

        def r4():
            ready(3)
            for k in range(2):
                for j in range(2):
                    edge(k, j).wait_recv()
            added(own.at[0], own.at[3], other.at[3], side.at[0], side.at[1])
            for k in range(4):
                swap(k).wait_send()
            for j in range(2):
                corner(j).wait_send()
            for k in range(2):
                for j in range(2):
                    edge(k, j).wait_send()
            if self.finish:
                far = scratch[7]
                over = move(10, own.at[0], far, "z")
                over.start()
                over.wait()
                added(own.at[1], own.at[0], far)
                save = pltpu.make_async_copy(own.at[1], result, local.at[4])
            else:
                save = pltpu.make_async_copy(own.at[0], result, local.at[4])
            save.start()
            save.wait()

        return list(zip(self.at, (r0, r1, r2, r3, r4)))


class Cross:
    def __init__(self, block, at):
        self.ins, self.outs, self.at = [block], [sds(block.shape)], at
        self.scratch = [pltpu.VMEM(block.shape, BF), pltpu.VMEM(block.shape, BF), DMA((2,)), DMA((1,)), DMA((1,))]

    def hooks(self, place, ins, outs, scratch):
        (block,), (result,), (mine, far, local, send, recv) = ins, outs, scratch
        over = lambda: pltpu.make_async_remote_copy(block, far, send.at[0], recv.at[0], device_id=place.dev["z"], device_id_type=MESH)
        load = lambda: pltpu.make_async_copy(block, mine, local.at[0])
        save = lambda: pltpu.make_async_copy(mine, result, local.at[1])

        def z0():
            over().start()
            load().start()

        def z1():
            load().wait()
            over().wait()
            added(mine, mine, far)
            save().start()
            save().wait()

        return list(zip(self.at, (z0, z1)))


def call(number, body, steps, ins, outs, args, scratch=(), comms=()):
    sizes = [(len(c.ins), len(c.outs), len(c.scratch)) for c in comms]
    nin, nout, nscr = len(ins), len(outs), len(scratch)

    def kernel(*refs):
        refs = list(refs)

        def take(n):
            got = refs[:n]
            del refs[:n]
            return got

        main_in = take(nin)
        c_in = [take(a) for a, _, _ in sizes]
        main_out = take(nout)
        c_out = [take(b) for _, b, _ in sizes]
        main_scr = take(nscr)
        c_scr = [take(c) for _, _, c in sizes]
        todo = []
        step = pl.program_id(0)
        if comms:
            place = Place()

            @pl.when(step == 0)
            def _():
                place.meet()

            for c, i, o, s in zip(comms, c_in, c_out, c_scr):
                todo += c.hooks(place, i, o, s)
        for k in range(steps):
            now = [f for at, f in todo if at == k]
            if now:

                @pl.when(step == k)
                def _(now=now):
                    for f in now:
                        f()

        if body is not None:
            body(*main_in, *main_out, *main_scr)
        last = [f for at, f in todo if at >= steps]
        if last:

            @pl.when(step == steps - 1)
            def _():
                for f in last:
                    f()

    c_args = [a for c in comms for a in c.ins]
    c_outs = [o for c in comms for o in c.outs]
    extra = dict(collective_id=number, has_side_effects=True) if comms else {}
    out = pl.pallas_call(
        kernel,
        grid=(steps,),
        in_specs=[*ins, *[ANY] * len(c_args)],
        out_specs=[*[o for o, _ in outs], *[ANY] * len(c_outs)],
        out_shape=[*[s for _, s in outs], *c_outs],
        scratch_shapes=[*scratch, *[s for c in comms for s in c.scratch]],
        compiler_params=pltpu.CompilerParams(vmem_limit_bytes=VMEM_LIMIT, dimension_semantics=("arbitrary",), **extra),
    )(*args, *c_args)
    return out[:nout], out[nout:]


def norm_tile(h):
    wide = h.astype(F32)
    scale = lax.rsqrt(jnp.mean(wide * wide, -1, keepdims=True) + 1e-6)
    return (wide * scale).astype(BF)


def up_body(x, wg, wu, a, gate, up, hidden):
    @pl.when(pl.program_id(0) == 0)
    def _():
        def one(m):
            a[m, :] = norm_tile(x[m, :])

        chunks(T, 256, one)

    def one(m):
        g, u = dot(a[m, :], wg[...]), dot(a[m, :], wu[...])
        gate[m, :], up[m, :] = g, u
        hidden[m, :] = (g * jax.nn.sigmoid(g) * u).astype(BF)

    chunks(T, MC, one)


def down_body(hidden, wd, x, h, a):
    new = x[...] + dot(hidden[...], wd[...]).astype(BF)
    h[...] = new
    a[...] = norm_tile(new)


def gates(g, u, dh):
    sig = jax.nn.sigmoid(g)
    return (dh * u * (sig * (1 + g * (1 - sig)))).astype(BF), (dh * (g * sig)).astype(BF)


def top_body(a, dy, wg, wu, wd, hidden, dgate, dup):
    def one(m):
        g, u = dot(a[m, :], wg[...]), dot(a[m, :], wu[...])
        dh = dot(dy[m, :], wd[...], 1, 1).astype(BF).astype(F32)
        hidden[m, :] = (g * jax.nn.sigmoid(g) * u).astype(BF)
        dgate[m, :], dup[m, :] = gates(g, u, dh)

    chunks(T, MC, one)


def wdown_body(hidden, dy, out):
    out[...] = dot(hidden[...], dy[...], 0, 0).astype(BF)


def low_body(dy, wd, gate, up, hidden, dgate, dup, out):
    def one(m):
        dh = dot(dy[m, :], wd[...], 1, 1).astype(BF).astype(F32)
        dgate[m, :], dup[m, :] = gates(gate[m, :], up[m, :], dh)

    chunks(T, MC, one)
    out[...] = dot(hidden[...], dy[...], 0, 0).astype(BF)


def wide_body(a, dgate, dup, og, ou, at):
    @pl.when(pl.program_id(0) == 0)
    def _():
        def one(m):
            at[:, m] = a[m, :].T

        chunks(T, 256, one)

    og[...] = dot(at[...], dgate[...]).astype(BF)
    ou[...] = dot(at[...], dup[...]).astype(BF)


def back_body(dgate, dup, wg, wu, h, dy, out):
    da = dot(dgate[...], wg[...], 1, 1) + dot(dup[...], wu[...], 1, 1)
    wide = h[...].astype(F32)
    scale = lax.rsqrt(jnp.mean(wide * wide, -1, keepdims=True) + 1e-6)
    inner = jnp.mean(da * wide, -1, keepdims=True)
    dh = scale * da - wide * (scale * scale * scale * inner)
    out[...] = (dy[...].astype(F32) + dh.astype(BF).astype(F32)).astype(BF)


def k_up(number, x, wg, wu, comms):
    wide = columns(T, TN)
    outs = [(resident((T, D)), sds((T, D))), (wide, sds((T, FF), F32)), (wide, sds((T, FF), F32)), (wide, sds((T, FF)))]
    return call(number, up_body, FF // TN, [resident((T, D)), columns(D, TN), columns(D, TN)], outs, (x, wg, wu), comms=comms)


def k_down(number, hidden, wd, x, comms):
    r = rows_of(TM, D)
    outs = [(r, sds((T, D))), (r, sds((T, D)))]
    return call(number, down_body, T // TM, [rows_of(TM, FF), resident((FF, D)), r], outs, (hidden, wd, x), comms=comms)


def k_top(number, a, dy, wg, wu, wd, comms):
    wide = columns(T, TN)
    ins = [resident((T, D)), resident((T, D)), columns(D, TN), columns(D, TN), rows_of(TN, D)]
    return call(number, top_body, FF // TN, ins, [(wide, sds((T, FF)))] * 3, (a, dy, wg, wu, wd), comms=comms)


def k_wdown(number, hidden, dy, comms):
    return call(number, wdown_body, FF // TN, [columns(T, TN), resident((T, D))], [(rows_of(TN, D), sds((FF, D)))], (hidden, dy), comms=comms)


def k_low(number, dy, wd, gate, up, hidden, comms):
    wide = columns(T, TN)
    ins = [resident((T, D)), rows_of(TN, D), wide, wide, wide]
    outs = [(wide, sds((T, FF))), (wide, sds((T, FF))), (rows_of(TN, D), sds((FF, D)))]
    return call(number, low_body, FF // TN, ins, outs, (dy, wd, gate, up, hidden), comms=comms)


def k_wide(number, a, dgate, dup, comms):
    ins = [resident((T, D)), columns(T, TN), columns(T, TN)]
    outs = [(columns(D, TN), sds((D, FF)))] * 2
    return call(number, wide_body, FF // TN, ins, outs, (a, dgate, dup), [pltpu.VMEM((D, T), BF)], comms=comms)


def k_back(number, dgate, dup, wg, wu, h, dy, comms):
    r = rows_of(TM, D)
    ins = [rows_of(TM, FF), rows_of(TM, FF), resident((D, FF)), resident((D, FF)), r, r]
    return call(number, back_body, T // TM, ins, [(r, sds((T, D)))], (dgate, dup, wg, wu, h, dy), comms=comms)


def k_comm(number, comms):
    return call(number, None, 1, [], [], (), comms=comms)[1]


SCATTER_AT = (0, 1, 2, 4, 8)
CROSS_AT = (0, 6)


def solution(mesh):
    def step(x, dy, wg, wu, wd):
        x, dy = x[0], dy[0]
        wg0, wu0 = k_comm(0, [Gather([wg, wu], [0, 0], gather_steps(2, lambda k: 0))])
        fetch = Gather([wd, wg, wu], [0, 1, 1], gather_steps(3, lambda k: (0, 2, 3, 5, 6, 8, 8)[k]))
        (a0, gate, up, hidden), (wd0, wg1, wu1) = k_up(1, x, wg0, wu0, [fetch])
        fetch = Gather([wd], [1], gather_steps(1, lambda k: (0, 6, 8, 8, 8)[k]))
        (h1, a1), (wd1,) = k_down(2, hidden, wd0, x, [fetch])
        (top, dgate, dup), _ = k_top(3, a1, dy, wg1, wu1, wd1, [])
        (td1,), _ = k_wdown(4, top, dy, [])
        (tg1, tu1), (pd1,) = k_wide(5, a1, dgate, dup, [Scatter(td1, SCATTER_AT)])
        (dh,), (pg1, od1) = k_back(6, dgate, dup, wg1, wu1, h1, dy, [Scatter(tg1, SCATTER_AT), Cross(pd1, CROSS_AT)])
        (dgate, dup, td0), (pu1, og1) = k_low(7, dh, wd0, gate, up, hidden, [Scatter(tu1, SCATTER_AT), Cross(pg1, CROSS_AT)])
        (tg0, tu0), (pd0, ou1) = k_wide(8, a0, dgate, dup, [Scatter(td0, SCATTER_AT), Cross(pu1, CROSS_AT)])
        (dx,), (pg0, od0) = k_back(9, dgate, dup, wg0, wu0, x, dh, [Scatter(tg0, SCATTER_AT), Cross(pd0, CROSS_AT)])
        ou0, og0 = k_comm(10, [Scatter(tu0, (0,) * 5, finish=True), Cross(pg0, (0, 0))])
        return dx[None], jnp.stack([og0, og1]), jnp.stack([ou0, ou1]), jnp.stack([od0, od1])

    states, cut = P(("rep", "r", "s"), None, None), P(None, "s", None)
    return jax.shard_map(
        step,
        mesh=mesh,
        in_specs=(states, states) + (cut,) * 3,
        out_specs=(states,) + (P("rep", "s", None),) * 3,
        check_vma=False,
    )
```

```python
import functools

import jax
import jax.numpy as jnp
from jax import lax
from jax.experimental import pallas as pl
from jax.experimental.pallas import tpu as pltpu
from jax.sharding import PartitionSpec as P

BF, F32 = jnp.bfloat16, jnp.float32
T, D, FF = 2048, 1024, 4096
TN, TM, MC = 512, 256, 1024
VMEM_LIMIT = 67043328
MESH = pl.DeviceIdType.MESH
DMA = pltpu.SemaphoreType.DMA
ANY = pl.BlockSpec(memory_space=pl.ANY)


def sds(shape, dtype=BF):
    return jax.ShapeDtypeStruct(shape, dtype)


def resident(shape):
    return pl.BlockSpec(shape, lambda i: (0, 0), pipeline_mode=pl.Buffered(1))


def columns(rows, cols):
    return pl.BlockSpec((rows, cols), lambda i: (0, i))


def rows_of(rows, cols):
    return pl.BlockSpec((rows, cols), lambda i: (i, 0))


def dot(a, b, ca=1, cb=0):
    return lax.dot_general(a, b, (((ca,), (cb,)), ((), ())), preferred_element_type=F32)


def chunks(total, size, f):
    def go(i, c):
        f(pl.ds(pl.multiple_of(i * size, size), size))
        return c

    lax.fori_loop(0, total // size, go, 0)


class Place:
    def __init__(self):
        self.rep, self.r, self.s = lax.axis_index("rep"), lax.axis_index("r"), lax.axis_index("s")
        s = self.s
        x, y, c = s // 4, (s // 2) % 2, s % 2
        at = lambda x, y, c: x * 4 + y * 2 + c
        self.sx, self.sy, self.sd, self.sc = at(1 - x, y, c), at(x, 1 - y, c), at(1 - x, 1 - y, c), at(x, y, 1 - c)
        self.order = [self.sd, self.sx, self.sy, s]
        self.across = [at(1 - x, 1 - y, 1 - c), at(1 - x, y, 1 - c), at(x, 1 - y, 1 - c), self.sc]
        self.dev = {
            "x": (self.rep, self.r, self.sx),
            "y": (self.rep, self.r, self.sy),
            "z": (self.rep, 1 - self.r, s),
            "c": (self.rep, self.r, self.sc),
        }

    def meet(self):
        barrier = pltpu.get_barrier_semaphore()
        for d in "xyzc":
            pl.semaphore_signal(barrier, inc=1, device_id=self.dev[d], device_id_type=MESH)
        pl.semaphore_wait(barrier, 4)


def rows_at(start, size, unit):
    return pl.ds(pl.multiple_of(start, unit), size)


class Gather:
    TAGS, PARTS = 17, 2

    def __init__(self, shards, layers, at):
        self.ins, self.layers, n = list(shards), layers, len(shards)
        self.outs = [sds((8 * a.shape[1], a.shape[2])) for a in shards]
        self.work = [(i, k) for i in range(0, n) for k in range(self.PARTS)]
        self.at, count = at, len(shards) * self.PARTS
        self.scratch = [pltpu.VMEM((a.shape[1], a.shape[2] // self.PARTS), BF) for a in shards for _ in range(self.PARTS)]
        self.scratch += [DMA((count, 2)), DMA((count, self.TAGS)), DMA((count, self.TAGS))]

    def reorder(self, work):
        self.work = work
        return self

    def hooks(self, place, ins, outs, scratch):
        p, count = place, len(self.work)
        bounce, (local, send, recv) = scratch[:count], scratch[count:]

        def moves(w):
            i, k = self.work[w]
            layer, width = self.layers[i], ins[i].shape[2] // self.PARTS
            over = pl.ds(k * width, width)
            shard, whole, own = ins[i], outs[i], bounce[i * self.PARTS + k]
            rows = shard.shape[1]
            n = rows // 4
            q = [k + p.r * (3 - 2 * k) for k in range(4)]
            slot = lambda owner, k: whole.at[rows_at(owner * rows + q[k] * n, n, n), over]
            three = lambda owner: whole.at[rows_at(owner * rows + p.r * n, 3 * n, n), over]
            direct = shard.at[layer, rows_at(p.r * n, 3 * n, n), over]
            all_mine, mine = shard.at[layer, :, over], whole.at[rows_at(p.s * rows, rows, rows), over]
            todo = [(direct, three(p.s), "x"), (direct, three(p.s), "y")]
            relay = [(slot(p.sy, 0), "x"), (slot(p.sx, 1), "y"), (slot(p.sx, 0), "z"), (slot(p.sy, 0), "z")]
            relay += [(slot(p.sd, 0), "z"), (slot(p.sd, 1), "z")]
            todo += [(a, a, d) for a, d in relay]
            todo += [(all_mine, mine, "c")]
            core = [three(p.sx), three(p.sy), slot(p.sd, 0), slot(p.sd, 1)]
            core += [slot(p.sx, 3), slot(p.sy, 3), slot(p.sd, 3), slot(p.sd, 2)]
            todo += [(a, a, "c") for a in core]

            def move(t):
                a, b, d = todo[t]
                return pltpu.make_async_remote_copy(a, b, send.at[w, t], recv.at[w, t], device_id=p.dev[d], device_id_type=MESH)

            load = lambda: pltpu.make_async_copy(all_mine, own, local.at[w, 0])
            save = lambda: pltpu.make_async_copy(own, mine, local.at[w, 1])
            return move, load, save

        def a0(i):
            m, load, _ = moves(i)
            for t in (0, 1, 8):
                m(t).start()
            load().start()

        def a1(i):
            m, load, save = moves(i)
            m(0).wait_recv()
            m(3).start()
            m(4).start()
            m(1).wait_recv()
            for t in (2, 5, 9, 10):
                m(t).start()
            load().wait()
            save().start()

        def a2(i):
            m, _, _ = moves(i)
            m(2).wait_recv()
            m(6).start()
            m(11).start()
            m(3).wait_recv()
            m(7).start()
            m(12).start()

        def a3(i):
            m, _, _ = moves(i)
            for t, u in ((4, 13), (5, 14), (6, 15), (7, 16)):
                m(t).wait_recv()
                m(u).start()

        def a4(i):
            m, _, save = moves(i)
            for t in range(8, 17):
                m(t).wait_recv()
            for t in range(17):
                m(t).wait_send()
            save().wait()

        ahead, out = 3, []

        def add(at, f, i):
            if 0 <= i < count:
                out.append((at, functools.partial(f, i)))

        for i in range(ahead):
            add(0, a0, i)
        for k in range(count + 3):
            at = self.at(k)
            for f, i in ((a1, k), (a0, k + ahead), (a2, k - 1), (a3, k - 2), (a4, k - 3)):
                if f is not a0 or i >= ahead:
                    add(at, f, i)
        return out


def added(out, *terms):
    rows, cols = out.shape
    size = 65536 // cols

    def one(m):
        total = terms[0][m, :].astype(F32)
        for t in terms[1:]:
            total += t[m, :].astype(F32)
        out[m, :] = total.astype(BF)

    chunks(rows, size, one)


class Scatter:
    def __init__(self, term, at, finish=False, part=(0, 1)):
        self.rows, self.cols, self.first = term.shape[0] // 8, term.shape[1] // part[1], term.shape[1] // part[1] * part[0]
        self.ins, self.at, self.finish = [term], at, finish
        self.outs = [sds((self.rows, self.cols))]
        block, half = (self.rows, self.cols), (self.rows // 2, self.cols)
        self.scratch = [pltpu.VMEM((4, *block), BF), pltpu.VMEM((4, *block), BF), pltpu.VMEM((2, *half), BF), pltpu.VMEM((2, *block), BF)]
        self.scratch += [DMA((5,)), DMA((11,)), DMA((11,))]
        if finish:
            self.scratch.append(pltpu.VMEM(block, BF))

    def hooks(self, place, ins, outs, scratch):
        p, (term,), (result,) = place, ins, outs
        own, other, diag, side, local, send, recv = scratch[:7]
        rows, h = self.rows, self.rows // 2
        block = lambda b: term.at[rows_at(b * rows, rows, rows), pl.ds(self.first, self.cols)]
        part = lambda ref, k, j: ref.at[k, pl.ds(j * h, h)]

        def move(t, a, b, d):
            return pltpu.make_async_remote_copy(a, b, send.at[t], recv.at[t], device_id=p.dev[d], device_id_type=MESH)

        swap = lambda k: move(k, block(p.across[k]), other.at[k], "c")
        load = lambda k: pltpu.make_async_copy(block(p.order[k]), own.at[k], local.at[k])
        corner = lambda j: move(4 + j, part(other, 0, j), diag.at[j], "xy"[j])
        edge = lambda k, j: move(6 + 2 * k + j, part(other, 1 + k, j), part(side, k, j), "xy"[k])
        over = lambda: move(10, own.at[0], scratch[7], "z")
        save = lambda k: pltpu.make_async_copy(own.at[k], result, local.at[4])

        def r0():
            for k in range(4):
                swap(k).start()
                load(k).start()

        def ready(k):
            swap(k).wait_recv()
            load(k).wait()

        def r1():
            ready(0)
            for j in range(2):
                added(part(other, 0, j), part(other, 0, j), part(own, 0, j))
                corner(j).start()

        def r2():
            for k in range(2):
                ready(1 + k)
                added(part(other, 1 + k, k), part(other, 1 + k, k), part(own, 1 + k, k))
                edge(k, k).start()

        def r3():
            for k in range(2):
                j = 1 - k
                corner(j).wait_recv()
                added(part(other, 1 + k, j), part(other, 1 + k, j), part(own, 1 + k, j), diag.at[j])
                edge(k, j).start()

        def r4():
            ready(3)
            for k in range(2):
                for j in range(2):
                    edge(k, j).wait_recv()
            added(own.at[0], own.at[3], other.at[3], side.at[0], side.at[1])
            if self.finish:
                over().start()
            else:
                save(0).start()
            for k in range(4):
                swap(k).wait_send()
            for j in range(2):
                corner(j).wait_send()
            for k in range(2):
                for j in range(2):
                    edge(k, j).wait_send()

        def r5():
            if self.finish:
                over().wait()
                added(own.at[1], own.at[0], scratch[7])
                save(1).start()

        def r6():
            save(0).wait()

        return list(zip(self.at, (r0, r1, r2, r3, r4, r5, r6)))


class Cross:
    def __init__(self, block, at):
        self.ins, self.outs, self.at = [block], [sds(block.shape)], at
        self.scratch = [pltpu.VMEM(block.shape, BF), pltpu.VMEM(block.shape, BF), DMA((2,)), DMA((1,)), DMA((1,))]

    def hooks(self, place, ins, outs, scratch):
        (block,), (result,), (mine, far, local, send, recv) = ins, outs, scratch
        over = lambda: pltpu.make_async_remote_copy(block, far, send.at[0], recv.at[0], device_id=place.dev["z"], device_id_type=MESH)
        load = lambda: pltpu.make_async_copy(block, mine, local.at[0])
        save = lambda: pltpu.make_async_copy(mine, result, local.at[1])

        def z0():
            over().start()
            load().start()

        def z1():
            load().wait()
            over().wait()
            added(mine, mine, far)
            save().start()
            save().wait()

        return list(zip(self.at, (z0, z1)))


def call(number, body, steps, ins, outs, args, scratch=(), comms=(), share=False):
    sizes = [(len(c.ins), len(c.outs), len(c.scratch)) for c in comms]
    nin, nout, nscr = len(ins), len(outs), len(scratch)

    def kernel(*refs):
        refs = list(refs)

        def take(n):
            got = refs[:n]
            del refs[:n]
            return got

        main_in = take(nin)
        c_in = [take(a) for a, _, _ in sizes]
        main_out = take(nout)
        c_out = [take(b) for _, b, _ in sizes]
        main_scr = take(nscr)
        c_scr = [take(c) for _, _, c in sizes]
        todo = []
        step = pl.program_id(0)
        if comms:
            place = Place()

            @pl.when(step == 0)
            def _():
                place.meet()

            for c, i, o, s in zip(comms, c_in, c_out, c_scr):
                todo += c.hooks(place, i, o, s)
        todo.sort(key=lambda t: t[0])
        for k in range(steps):
            now = [f for at, f in todo if k <= at < k + 1]
            if now:

                @pl.when(step == k)
                def _(now=now):
                    for f in now:
                        f()

        if body is not None:
            body(*main_in, *main_out, *main_scr, *([c_out[0]] if share else []))
        last = [f for at, f in todo if at >= steps]
        if last:

            @pl.when(step == steps - 1)
            def _():
                for f in last:
                    f()

    c_args = [a for c in comms for a in c.ins]
    c_outs = [o for c in comms for o in c.outs]
    extra = dict(collective_id=number, has_side_effects=True) if comms else {}
    out = pl.pallas_call(
        kernel,
        grid=(steps,),
        in_specs=[*ins, *[ANY] * len(c_args)],
        out_specs=[*[o for o, _ in outs], *[ANY] * len(c_outs)],
        out_shape=[*[s for _, s in outs], *c_outs],
        scratch_shapes=[*scratch, *[s for c in comms for s in c.scratch]],
        compiler_params=pltpu.CompilerParams(vmem_limit_bytes=VMEM_LIMIT, dimension_semantics=("arbitrary",), **extra),
    )(*args, *c_args)
    return out[:nout], out[nout:]


def norm_tile(h):
    wide = h.astype(F32)
    scale = lax.rsqrt(jnp.mean(wide * wide, -1, keepdims=True) + 1e-6)
    return (wide * scale).astype(BF)


UT = 256
UPS = FF // UT


def first_body(x, a, gate, up, hidden, h, a1, g_buf, u_buf, kept, wd, sems, wd_sem, wholes):
    step = pl.program_id(0)
    fetch = lambda tile: [
        pltpu.make_async_copy(whole.at[:, rows_at(tile * UT, UT, UT)], buf.at[tile % 2], sems.at[k, tile % 2])
        for k, (whole, buf) in enumerate(((wholes[0], g_buf), (wholes[1], u_buf)))
    ]
    fetch_down = lambda: pltpu.make_async_copy(wholes[2], wd, wd_sem.at[0])

    @pl.when(step == 0)
    def _():
        for c in fetch(0):
            c.start()

        def one(m):
            a[m, :] = norm_tile(x[m, :])

        chunks(T, 256, one)

    @pl.when(step < UPS)
    def _():
        for c in fetch(step):
            c.wait()

        @pl.when(step < UPS - 1)
        def _():
            for c in fetch(step + 1):
                c.start()

        @pl.when(step == UPS - 1)
        def _():
            fetch_down().start()

        def one(m):
            g, u = dot(a[m, :], g_buf[step % 2]), dot(a[m, :], u_buf[step % 2])
            gate[m, :], up[m, :] = g, u
            made = (g * jax.nn.sigmoid(g) * u).astype(BF)
            hidden[m, :] = made
            kept[m, rows_at(step * UT, UT, UT)] = made

        chunks(T, MC, one)

    @pl.when(step == UPS)
    def _():
        fetch_down().wait()

    @pl.when(step >= UPS)
    def _():
        m = rows_at((step - UPS) * TM, TM, TM)
        new = x[m, :] + dot(kept[m, :], wd[...]).astype(BF)
        h[...] = new
        a1[...] = norm_tile(new)


def gates(g, u, dh):
    sig = jax.nn.sigmoid(g)
    return (dh * u * (sig * (1 + g * (1 - sig)))).astype(BF), (dh * (g * sig)).astype(BF)


def top_body(a, dy, wg, wu, wd, hidden, dgate, dup):
    def one(m):
        g, u = dot(a[m, :], wg[...]), dot(a[m, :], wu[...])
        dh = dot(dy[m, :], wd[...], 1, 1).astype(BF).astype(F32)
        hidden[m, :] = (g * jax.nn.sigmoid(g) * u).astype(BF)
        dgate[m, :], dup[m, :] = gates(g, u, dh)

    chunks(T, MC, one)


def wdown_body(hidden, dy, out):
    out[...] = dot(hidden[...], dy[...], 0, 0).astype(BF)


def low_body(dy, wd, gate, up, hidden, dgate, dup, out):
    def one(m):
        dh = dot(dy[m, :], wd[...], 1, 1).astype(BF).astype(F32)
        dgate[m, :], dup[m, :] = gates(gate[m, :], up[m, :], dh)

    chunks(T, MC, one)
    out[...] = dot(hidden[...], dy[...], 0, 0).astype(BF)


def wide_body(a, dgate, dup, og, ou, at):
    @pl.when(pl.program_id(0) == 0)
    def _():
        def one(m):
            at[:, m] = a[m, :].T

        chunks(T, 256, one)

    og[...] = dot(at[...], dgate[...]).astype(BF)
    ou[...] = dot(at[...], dup[...]).astype(BF)


def back_body(dgate, dup, wg, wu, h, dy, out):
    da = dot(dgate[...], wg[...], 1, 1) + dot(dup[...], wu[...], 1, 1)
    wide = h[...].astype(F32)
    scale = lax.rsqrt(jnp.mean(wide * wide, -1, keepdims=True) + 1e-6)
    inner = jnp.mean(da * wide, -1, keepdims=True)
    dh = scale * da - wide * (scale * scale * scale * inner)
    out[...] = (dy[...].astype(F32) + dh.astype(BF).astype(F32)).astype(BF)


def k_first(number, x, gather):
    wide = pl.BlockSpec((T, UT), lambda i: (0, jnp.minimum(i, UPS - 1)))
    r = pl.BlockSpec((TM, D), lambda i: (jnp.maximum(i - UPS, 0), 0))
    outs = [(resident((T, D)), sds((T, D))), (wide, sds((T, FF), F32)), (wide, sds((T, FF), F32)), (wide, sds((T, FF)))]
    outs += [(r, sds((T, D))), (r, sds((T, D)))]
    scratch = [pltpu.VMEM((2, D, UT), BF), pltpu.VMEM((2, D, UT), BF), pltpu.VMEM((T, FF), BF), pltpu.VMEM((FF, D), BF), DMA((2, 2)), DMA((1,))]
    return call(number, first_body, UPS + T // TM, [resident((T, D))], outs, (x,), scratch, comms=[gather], share=True)


def k_top(number, a, dy, wg, wu, wd, comms):
    wide = columns(T, TN)
    ins = [resident((T, D)), resident((T, D)), columns(D, TN), columns(D, TN), rows_of(TN, D)]
    return call(number, top_body, FF // TN, ins, [(wide, sds((T, FF)))] * 3, (a, dy, wg, wu, wd), comms=comms)


def k_wdown(number, hidden, dy, comms):
    return call(number, wdown_body, FF // TN, [columns(T, TN), resident((T, D))], [(rows_of(TN, D), sds((FF, D)))], (hidden, dy), comms=comms)


def k_low(number, dy, wd, gate, up, hidden, comms):
    wide = columns(T, TN)
    ins = [resident((T, D)), rows_of(TN, D), wide, wide, wide]
    outs = [(wide, sds((T, FF))), (wide, sds((T, FF))), (rows_of(TN, D), sds((FF, D)))]
    return call(number, low_body, FF // TN, ins, outs, (dy, wd, gate, up, hidden), comms=comms)


def k_wide(number, a, dgate, dup, comms):
    ins = [resident((T, D)), columns(T, TN), columns(T, TN)]
    outs = [(columns(D, TN), sds((D, FF)))] * 2
    return call(number, wide_body, FF // TN, ins, outs, (a, dgate, dup), [pltpu.VMEM((D, T), BF)], comms=comms)


def k_back(number, dgate, dup, wg, wu, h, dy, comms):
    r = rows_of(TM, D)
    ins = [rows_of(TM, FF), rows_of(TM, FF), resident((D, FF)), resident((D, FF)), r, r]
    return call(number, back_body, T // TM, ins, [(r, sds((T, D)))], (dgate, dup, wg, wu, h, dy), comms=comms)


def k_comm(number, comms):
    return call(number, None, 1, [], [], (), comms=comms)[1]


SCATTER_AT = (0, 1, 2, 4, 8, 8, 8)
CROSS_AT = (0, 6)


def solution(mesh):
    def step(x, dy, wg, wu, wd):
        x, dy = x[0], dy[0]
        when = (0, 0, 0, 0, 0, 3, 6, 9, 12, 15, 18, 21, 24, 24.1, 24.2)
        gather = Gather([wg, wu, wd, wg, wu, wd], [0, 0, 0, 1, 1, 1], lambda k: when[k])
        gather.reorder([(0, 0), (1, 0), (0, 1), (1, 1), *[(i, k) for i in range(2, 6) for k in range(2)]])
        (a0, gate, up, hidden, h1, a1), (wg0, wu0, wd0, wg1, wu1, wd1) = k_first(0, x, gather)
        (top, dgate, dup), _ = k_top(3, a1, dy, wg1, wu1, wd1, [])
        (td1,), _ = k_wdown(4, top, dy, [])
        (tg1, tu1), (pd1,) = k_wide(5, a1, dgate, dup, [Scatter(td1, SCATTER_AT)])
        (dh,), (pg1, od1) = k_back(6, dgate, dup, wg1, wu1, h1, dy, [Scatter(tg1, SCATTER_AT), Cross(pd1, CROSS_AT)])
        (dgate, dup, td0), (pu1, og1) = k_low(7, dh, wd0, gate, up, hidden, [Scatter(tu1, SCATTER_AT), Cross(pg1, CROSS_AT)])
        (tg0, tu0), (pd0, ou1) = k_wide(8, a0, dgate, dup, [Scatter(td0, SCATTER_AT), Cross(pu1, CROSS_AT)])
        last = [
            Cross(pd0, CROSS_AT),
            Scatter(tg0, (0, 1, 1.1, 3, 7, 8.25, 8.7), True),
            Scatter(tu0, (1.2, 4, 4.1, 8, 8.2, 8.4, 8.8), True, (0, 2)),
            Scatter(tu0, (2, 5, 8.05, 8.1, 8.3, 8.5, 8.9), True, (1, 2)),
        ]
        (dx,), (od0, og0, *ou0) = k_back(9, dgate, dup, wg0, wu0, x, dh, last)
        ou0 = jnp.concatenate(ou0, 1)
        return dx[None], jnp.stack([og0, og1]), jnp.stack([ou0, ou1]), jnp.stack([od0, od1])

    states, cut = P(("rep", "r", "s"), None, None), P(None, "s", None)
    return jax.shard_map(
        step,
        mesh=mesh,
        in_specs=(states, states) + (cut,) * 3,
        out_specs=(states,) + (P("rep", "s", None),) * 3,
        check_vma=False,
    )
```

```python
import functools

import jax
import jax.numpy as jnp
from jax import lax
from jax.experimental import pallas as pl
from jax.experimental.pallas import tpu as pltpu
from jax.sharding import PartitionSpec as P

BF, F32 = jnp.bfloat16, jnp.float32
T, D, FF = 2048, 1024, 4096
TN, TM, MC = 512, 256, 1024
VMEM_LIMIT = 67043328
AHEAD, LAGS, PARTS = 3, (2, 4, 6), 4
MESH = pl.DeviceIdType.MESH
DMA = pltpu.SemaphoreType.DMA
ANY = pl.BlockSpec(memory_space=pl.ANY)


def sds(shape, dtype=BF):
    return jax.ShapeDtypeStruct(shape, dtype)


def resident(shape):
    return pl.BlockSpec(shape, lambda i: (0, 0), pipeline_mode=pl.Buffered(1))


def columns(rows, cols):
    return pl.BlockSpec((rows, cols), lambda i: (0, i))


def rows_of(rows, cols):
    return pl.BlockSpec((rows, cols), lambda i: (i, 0))


def dot(a, b, ca=1, cb=0):
    return lax.dot_general(a, b, (((ca,), (cb,)), ((), ())), preferred_element_type=F32)


def chunks(total, size, f):
    def go(i, c):
        f(pl.ds(pl.multiple_of(i * size, size), size))
        return c

    lax.fori_loop(0, total // size, go, 0)


class Place:
    def __init__(self):
        self.rep, self.r, self.s = lax.axis_index("rep"), lax.axis_index("r"), lax.axis_index("s")
        s = self.s
        x, y, c = s // 4, (s // 2) % 2, s % 2
        at = lambda x, y, c: x * 4 + y * 2 + c
        self.sx, self.sy, self.sd, self.sc = at(1 - x, y, c), at(x, 1 - y, c), at(1 - x, 1 - y, c), at(x, y, 1 - c)
        self.order = [self.sd, self.sx, self.sy, s]
        self.across = [at(1 - x, 1 - y, 1 - c), at(1 - x, y, 1 - c), at(x, 1 - y, 1 - c), self.sc]
        self.dev = {
            "x": (self.rep, self.r, self.sx),
            "y": (self.rep, self.r, self.sy),
            "z": (self.rep, 1 - self.r, s),
            "c": (self.rep, self.r, self.sc),
        }

    def meet(self):
        barrier = pltpu.get_barrier_semaphore()
        for d in "xyzc":
            pl.semaphore_signal(barrier, inc=1, device_id=self.dev[d], device_id_type=MESH)
        pl.semaphore_wait(barrier, 4)


def rows_at(start, size, unit):
    return pl.ds(pl.multiple_of(start, unit), size)


class Gather:
    TAGS, PARTS = 18, PARTS

    def __init__(self, shards, layers, at):
        self.ins, self.layers, n = list(shards), layers, len(shards)
        self.outs = [sds((8 * a.shape[1], a.shape[2])) for a in shards]
        self.work = [(i, k) for i in range(0, n) for k in range(self.PARTS)]
        self.at, count = at, len(shards) * self.PARTS
        self.scratch = [DMA((count, self.TAGS)), DMA((count, self.TAGS))]

    def reorder(self, work):
        self.work = work
        return self

    def hooks(self, place, ins, outs, scratch):
        p, count = place, len(self.work)
        send, recv = scratch

        def moves(w):
            i, k = self.work[w]
            layer, width = self.layers[i], ins[i].shape[2] // self.PARTS
            over = pl.ds(k * width, width)
            shard, whole = ins[i], outs[i]
            rows = shard.shape[1]
            n = rows // 4
            q = [k + p.r * (3 - 2 * k) for k in range(4)]
            slot = lambda owner, k: whole.at[rows_at(owner * rows + q[k] * n, n, n), over]
            three = lambda owner: whole.at[rows_at(owner * rows + p.r * n, 3 * n, n), over]
            direct = shard.at[layer, rows_at(p.r * n, 3 * n, n), over]
            all_mine, mine = shard.at[layer, :, over], whole.at[rows_at(p.s * rows, rows, rows), over]
            todo = [(direct, three(p.s), "x"), (direct, three(p.s), "y")]
            relay = [(slot(p.sy, 0), "x"), (slot(p.sx, 1), "y"), (slot(p.sx, 0), "z"), (slot(p.sy, 0), "z")]
            relay += [(slot(p.sd, 0), "z"), (slot(p.sd, 1), "z")]
            todo += [(a, a, d) for a, d in relay]
            todo += [(all_mine, mine, "c")]
            core = [three(p.sx), three(p.sy), slot(p.sd, 0), slot(p.sd, 1)]
            core += [slot(p.sx, 3), slot(p.sy, 3), slot(p.sd, 3), slot(p.sd, 2)]
            theirs = whole.at[rows_at(p.sc * rows, rows, rows), over]
            todo += [(a, a, "c") for a in [*core, theirs]]

            def move(t):
                a, b, d = todo[t]
                return pltpu.make_async_remote_copy(a, b, send.at[w, t], recv.at[w, t], device_id=p.dev[d], device_id_type=MESH)

            return move

        def a0(i):
            m = moves(i)
            for t in (0, 1, 8):
                m(t).start()

        def a1(i):
            m = moves(i)
            m(0).wait_recv()
            m(3).start()
            m(4).start()
            m(1).wait_recv()
            for t in (2, 5, 9, 10):
                m(t).start()
            m(8).wait_recv()
            m(17).start()

        def a2(i):
            m = moves(i)
            m(2).wait_recv()
            m(6).start()
            m(11).start()
            m(3).wait_recv()
            m(7).start()
            m(12).start()

        def a3(i):
            m = moves(i)
            for t, u in ((4, 13), (5, 14), (6, 15), (7, 16)):
                m(t).wait_recv()
                m(u).start()

        def a4(i):
            m = moves(i)
            for t in range(9, 18):
                m(t).wait_recv()
            for t in range(18):
                m(t).wait_send()

        out = []

        def add(at, f, i):
            if 0 <= i < count:
                out.append((at, functools.partial(f, i)))

        for i in range(AHEAD):
            add(0, a0, i)
        for k in range(count + LAGS[2]):
            at = self.at[k]
            add(at, a1, k)
            add(at, a0, k + AHEAD)
            for f, lag in zip((a2, a3, a4), LAGS):
                add(at, f, k - lag)
        return out


def gather_times():
    work = [(m, k) for pair in ((0, 1), (2,), (5,), (3, 4)) for k in range(PARTS) for m in pair]
    one, each = 22.5 / PARTS, UPS // PARTS
    first = one * (2 + LAGS[2]) + 8
    starts = [first + 3.5 * min(i, UPS) + 3 * min(max(i - UPS, 0), DOWNS) + 5.2 * max(i - TOP, 0) for i in range(TOP + UPS)]
    need = {0: lambda k: max(each * k - 1, 0), 1: lambda k: max(each * k - 1, 0), 2: lambda k: UPS - 1, 5: lambda k: TOP}
    need[3] = need[4] = lambda k: TOP + max(each * k - 1, 0)
    total, when, cap = len(work) + LAGS[2], [], TOP + UPS - 1
    for k in reversed(range(total)):
        if k >= LAGS[2]:
            m, part = work[k - LAGS[2]]
            cap = min(cap, need[m](part))
        arrives = one * (k + 1) + 8
        late = [i for i, t in enumerate(starts) if t >= arrives - 1]
        when.append(min([cap, *late[:1]]))
    return work, when[::-1]


def added(out, *terms):
    rows, cols = out.shape
    size = 65536 // cols

    def one(m):
        total = terms[0][m, :].astype(F32)
        for t in terms[1:]:
            total += t[m, :].astype(F32)
        out[m, :] = total.astype(BF)

    chunks(rows, size, one)


class Scatter:
    def __init__(self, term, at, finish=False, part=(0, 1)):
        self.rows, self.cols, self.first = term.shape[0] // 8, term.shape[1] // part[1], term.shape[1] // part[1] * part[0]
        self.ins, self.at, self.finish = [term], at, finish
        self.outs = [sds((self.rows, self.cols))]
        block, half = (self.rows, self.cols), (self.rows // 2, self.cols)
        self.scratch = [pltpu.VMEM((4, *block), BF), pltpu.VMEM((4, *block), BF), pltpu.VMEM((2, *half), BF), pltpu.VMEM((2, *block), BF)]
        self.scratch += [DMA((5,)), DMA((11,)), DMA((11,))]
        if finish:
            self.scratch.append(pltpu.VMEM(block, BF))

    def hooks(self, place, ins, outs, scratch):
        p, (term,), (result,) = place, ins, outs
        own, other, diag, side, local, send, recv = scratch[:7]
        rows, h = self.rows, self.rows // 2
        block = lambda b: term.at[rows_at(b * rows, rows, rows), pl.ds(self.first, self.cols)]
        part = lambda ref, k, j: ref.at[k, pl.ds(j * h, h)]

        def move(t, a, b, d):
            return pltpu.make_async_remote_copy(a, b, send.at[t], recv.at[t], device_id=p.dev[d], device_id_type=MESH)

        swap = lambda k: move(k, block(p.across[k]), other.at[k], "c")
        load = lambda k: pltpu.make_async_copy(block(p.order[k]), own.at[k], local.at[k])
        corner = lambda j: move(4 + j, part(other, 0, j), diag.at[j], "xy"[j])
        edge = lambda k, j: move(6 + 2 * k + j, part(other, 1 + k, j), part(side, k, j), "xy"[k])
        over = lambda: move(10, own.at[0], scratch[7], "z")
        save = lambda k: pltpu.make_async_copy(own.at[k], result, local.at[4])

        def r0():
            for k in range(4):
                swap(k).start()
                load(k).start()

        def ready(k):
            swap(k).wait_recv()
            load(k).wait()

        def r1():
            ready(0)
            for j in range(2):
                added(part(other, 0, j), part(other, 0, j), part(own, 0, j))
                corner(j).start()

        def r2():
            for k in range(2):
                ready(1 + k)
                added(part(other, 1 + k, k), part(other, 1 + k, k), part(own, 1 + k, k))
                edge(k, k).start()

        def r3():
            for k in range(2):
                j = 1 - k
                corner(j).wait_recv()
                added(part(other, 1 + k, j), part(other, 1 + k, j), part(own, 1 + k, j), diag.at[j])
                edge(k, j).start()

        def r4():
            ready(3)
            for k in range(2):
                for j in range(2):
                    edge(k, j).wait_recv()
            added(own.at[0], own.at[3], other.at[3], side.at[0], side.at[1])
            if self.finish:
                over().start()
            else:
                save(0).start()
            for k in range(4):
                swap(k).wait_send()
            for j in range(2):
                corner(j).wait_send()
            for k in range(2):
                for j in range(2):
                    edge(k, j).wait_send()

        def r5():
            if self.finish:
                over().wait()
                added(own.at[1], own.at[0], scratch[7])
                save(1).start()

        def r6():
            save(0).wait()

        return list(zip(self.at, (r0, r1, r2, r3, r4, r5, r6)))


class Cross:
    def __init__(self, block, at):
        self.ins, self.outs, self.at = [block], [sds(block.shape)], at
        self.scratch = [pltpu.VMEM(block.shape, BF), pltpu.VMEM(block.shape, BF), DMA((2,)), DMA((1,)), DMA((1,))]

    def hooks(self, place, ins, outs, scratch):
        (block,), (result,), (mine, far, local, send, recv) = ins, outs, scratch
        over = lambda: pltpu.make_async_remote_copy(block, far, send.at[0], recv.at[0], device_id=place.dev["z"], device_id_type=MESH)
        load = lambda: pltpu.make_async_copy(block, mine, local.at[0])
        save = lambda: pltpu.make_async_copy(mine, result, local.at[1])

        def z0():
            over().start()
            load().start()

        def z1():
            load().wait()
            over().wait()
            added(mine, mine, far)
            save().start()
            save().wait()

        return list(zip(self.at, (z0, z1)))


def call(number, body, steps, ins, outs, args, scratch=(), comms=(), share=False, early=None):
    sizes = [(len(c.ins), len(c.outs), len(c.scratch)) for c in comms]
    nin, nout, nscr = len(ins), len(outs), len(scratch)

    def kernel(*refs):
        refs = list(refs)

        def take(n):
            got = refs[:n]
            del refs[:n]
            return got

        main_in = take(nin)
        c_in = [take(a) for a, _, _ in sizes]
        main_out = take(nout)
        c_out = [take(b) for _, b, _ in sizes]
        main_scr = take(nscr)
        c_scr = [take(c) for _, _, c in sizes]
        todo = []
        step = pl.program_id(0)
        if early is not None:

            @pl.when(step == 0)
            def _():
                early(*main_in, *main_out, *main_scr)

        if comms:
            place = Place()

            @pl.when(step == 0)
            def _():
                place.meet()

            for c, i, o, s in zip(comms, c_in, c_out, c_scr):
                todo += c.hooks(place, i, o, s)
        todo.sort(key=lambda t: t[0])
        for k in range(steps):
            now = [f for at, f in todo if k <= at < k + 1]
            if now:

                @pl.when(step == k)
                def _(now=now):
                    for f in now:
                        f()

        if body is not None:
            body(*main_in, *main_out, *main_scr, *([c_out[0]] if share else []))
        last = [f for at, f in todo if at >= steps]
        if last:

            @pl.when(step == steps - 1)
            def _():
                for f in last:
                    f()

    c_args = [a for c in comms for a in c.ins]
    c_outs = [o for c in comms for o in c.outs]
    extra = dict(collective_id=number, has_side_effects=True) if comms else {}
    out = pl.pallas_call(
        kernel,
        grid=(steps,),
        in_specs=[*ins, *[ANY] * len(c_args)],
        out_specs=[*[o for o, _ in outs], *[ANY] * len(c_outs)],
        out_shape=[*[s for _, s in outs], *c_outs],
        scratch_shapes=[*scratch, *[s for c in comms for s in c.scratch]],
        compiler_params=pltpu.CompilerParams(vmem_limit_bytes=VMEM_LIMIT, dimension_semantics=("arbitrary",), **extra),
    )(*args, *c_args)
    return out[:nout], out[nout:]


def norm_tile(h):
    wide = h.astype(F32)
    scale = lax.rsqrt(jnp.mean(wide * wide, -1, keepdims=True) + 1e-6)
    return (wide * scale).astype(BF)


UT = 256
UPS, DOWNS = FF // UT, T // TM
TOP = UPS + DOWNS


def first_body(x, dy, a, gate, up, hidden, h, a1, dgate, dup, td, g_buf, u_buf, kept, wd, states, made, sems, one_sem, wholes):
    step = pl.program_id(0)

    def tile_of(k, tile):
        cols = rows_at(tile * UT, UT, UT)
        pairs = [(wholes[k].at[:, cols], g_buf), (wholes[k + 1].at[:, cols], u_buf)]
        return [pltpu.make_async_copy(w, buf.at[tile % 2], sems.at[j, tile % 2]) for j, (w, buf) in enumerate(pairs)]

    def top_tile(tile):
        rows = rows_at(tile * UT, UT, UT)
        return [*tile_of(3, tile), pltpu.make_async_copy(wholes[5].at[rows], wd.at[rows], sems.at[2, tile % 2])]

    fetch_down = lambda: pltpu.make_async_copy(wholes[2], wd, one_sem.at[0])
    fetch_x = lambda: pltpu.make_async_copy(x, states, one_sem.at[1])
    fetch_dy = lambda: pltpu.make_async_copy(dy, states, one_sem.at[2])

    def start(copies):
        for c in copies:
            c.start()

    def wait(copies):
        for c in copies:
            c.wait()

    @pl.when(step == 0)
    def _():
        start([*tile_of(0, 0), fetch_x()])
        fetch_x().wait()

        def one(m):
            a[m, :] = norm_tile(states[m, :])

        chunks(T, 256, one)

    @pl.when(step < UPS)
    def _():
        wait(tile_of(0, step))

        @pl.when(step < UPS - 1)
        def _():
            start(tile_of(0, step + 1))

        @pl.when(step == UPS - 1)
        def _():
            fetch_down().start()

        def one(m):
            g, u = dot(a[m, :], g_buf[step % 2]), dot(a[m, :], u_buf[step % 2])
            gate[m, :], up[m, :] = g, u
            product = (g * jax.nn.sigmoid(g) * u).astype(BF)
            hidden[m, :] = product
            kept[m, rows_at(step * UT, UT, UT)] = product

        chunks(T, 1024, one)

    @pl.when(step == UPS)
    def _():
        fetch_down().wait()

    @pl.when((step >= UPS) & (step < TOP))
    def _():
        m = rows_at((step - UPS) * TM, TM, TM)
        new = states[m, :] + dot(kept[m, :], wd[...]).astype(BF)
        h[...] = new
        a1[m, :] = norm_tile(new)

    @pl.when(step == TOP)
    def _():
        start([*top_tile(0), fetch_dy()])
        fetch_dy().wait()

    @pl.when(step >= TOP)
    def _():
        tile = step - TOP
        wait(top_tile(tile))

        @pl.when(tile < UPS - 1)
        def _():
            start(top_tile(tile + 1))

        down = rows_at(tile * UT, UT, UT)

        def one(m):
            g, u = dot(a1[m, :], g_buf[tile % 2]), dot(a1[m, :], u_buf[tile % 2])
            dh = dot(states[m, :], wd[down, :], 1, 1).astype(BF).astype(F32)
            made[m, :] = (g * jax.nn.sigmoid(g) * u).astype(BF)
            dgate[m, :], dup[m, :] = gates(g, u, dh)

        chunks(T, 1024, one)
        td[...] = dot(made[...], states[...], 0, 0).astype(BF)


def gates(g, u, dh):
    sig = jax.nn.sigmoid(g)
    return (dh * u * (sig * (1 + g * (1 - sig)))).astype(BF), (dh * (g * sig)).astype(BF)


def low_body(dy, wd, gate, up, hidden, dgate, dup, out):
    for k in range(T // 256):
        m = pl.ds(k * 256, 256)
        dh = dot(dy[m, :], wd[...], 1, 1).astype(BF).astype(F32)
        dgate[m, :], dup[m, :] = gates(gate[m, :], up[m, :], dh)
    out[...] = dot(hidden[...], dy[...], 0, 0).astype(BF)


def wide_body(a, dgate, dup, og, ou, at):
    @pl.when(pl.program_id(0) == 0)
    def _():
        def one(m):
            at[:, m] = a[m, :].T

        chunks(T, 256, one)

    og[...] = dot(at[...], dgate[...]).astype(BF)
    ou[...] = dot(at[...], dup[...]).astype(BF)


def back_loads(wg, wu, gs, us, sems):
    out = []
    for k in range(4):
        c = pl.ds(k * D, D)
        out.append([pltpu.make_async_copy(w.at[:, c], v.at[:, c], sems.at[j, k]) for j, (w, v) in enumerate(((wg, gs), (wu, us)))])
    return out


def back_early(dgate, dup, wg, wu, h, dy, out, gs, us, da, sems):
    for pair in back_loads(wg, wu, gs, us, sems):
        for c in pair:
            c.start()


def back_body(dgate, dup, wg, wu, h, dy, out, gs, us, da, sems):
    first = pl.program_id(0) == 0

    @pl.when(first)
    def _():
        for k, pair in enumerate(back_loads(wg, wu, gs, us, sems)):
            for c in pair:
                c.wait()
            c = pl.ds(k * D, D)
            more = dot(dgate[:, c], gs[:, c], 1, 1) + dot(dup[:, c], us[:, c], 1, 1)
            da[...] = more if k == 0 else da[...] + more

    @pl.when(jnp.logical_not(first))
    def _():
        da[...] = dot(dgate[...], gs[...], 1, 1) + dot(dup[...], us[...], 1, 1)

    wide, total = h[...].astype(F32), da[...]
    scale = lax.rsqrt(jnp.mean(wide * wide, -1, keepdims=True) + 1e-6)
    inner = jnp.mean(total * wide, -1, keepdims=True)
    dh = scale * total - wide * (scale * scale * scale * inner)
    out[...] = (dy[...].astype(F32) + dh.astype(BF).astype(F32)).astype(BF)


def k_first(number, x, dy, gather):
    wide = pl.BlockSpec((T, UT), lambda i: (0, jnp.minimum(i, UPS - 1)))
    late = pl.BlockSpec((T, UT), lambda i: (0, jnp.maximum(i - TOP, 0)))
    r = pl.BlockSpec((TM, D), lambda i: (jnp.clip(i - UPS, 0, DOWNS - 1), 0))
    outs = [(resident((T, D)), sds((T, D))), (wide, sds((T, FF), F32)), (wide, sds((T, FF), F32)), (wide, sds((T, FF)))]
    outs += [(r, sds((T, D))), (resident((T, D)), sds((T, D))), (late, sds((T, FF))), (late, sds((T, FF)))]
    outs += [(pl.BlockSpec((UT, D), lambda i: (jnp.maximum(i - TOP, 0), 0)), sds((FF, D)))]
    scratch = [pltpu.VMEM((2, D, UT), BF), pltpu.VMEM((2, D, UT), BF), pltpu.VMEM((T, FF), BF), pltpu.VMEM((FF, D), BF)]
    scratch += [pltpu.VMEM((T, D), BF), pltpu.VMEM((T, UT), BF), DMA((3, 2)), DMA((3,))]
    return call(number, first_body, TOP + UPS, [ANY, ANY], outs, (x, dy), scratch, comms=[gather], share=True)


def k_low(number, dy, wd, gate, up, hidden, comms):
    wide = columns(T, UT)
    ins = [resident((T, D)), rows_of(UT, D), wide, wide, wide]
    outs = [(wide, sds((T, FF))), (wide, sds((T, FF))), (rows_of(UT, D), sds((FF, D)))]
    return call(number, low_body, UPS, ins, outs, (dy, wd, gate, up, hidden), comms=comms)


def k_wide(number, a, dgate, dup, comms):
    ins = [resident((T, D)), columns(T, TN), columns(T, TN)]
    outs = [(columns(D, TN), sds((D, FF)))] * 2
    return call(number, wide_body, FF // TN, ins, outs, (a, dgate, dup), [pltpu.VMEM((D, T), BF)], comms=comms)


def k_back(number, dgate, dup, wg, wu, h, dy, comms):
    r = rows_of(TM, D)
    ins = [rows_of(TM, FF), rows_of(TM, FF), ANY, ANY, r, r]
    scratch = [pltpu.VMEM((D, FF), BF), pltpu.VMEM((D, FF), BF), pltpu.VMEM((TM, D), F32), DMA((2, 4))]
    outs = [(r, sds((T, D)))]
    return call(number, back_body, T // TM, ins, outs, (dgate, dup, wg, wu, h, dy), scratch, comms=comms, early=back_early)


def k_comm(number, comms):
    return call(number, None, 1, [], [], (), comms=comms)[1]


SCATTER_AT = (0, 0.1, 1, 3, 8, 8, 8)
CROSS_AT = (0, 6)


def solution(mesh):
    def step(x, dy, wg, wu, wd):
        x, dy = x[0], dy[0]
        work, when = gather_times()
        gather = Gather([wg, wu, wd, wg, wu, wd], [0, 0, 0, 1, 1, 1], when).reorder(work)
        (a0, gate, up, hidden, h1, a1, dgate, dup, td1), (wg0, wu0, wd0, wg1, wu1, wd1) = k_first(0, x, dy, gather)
        (tg1, tu1), (pd1,) = k_wide(5, a1, dgate, dup, [Scatter(td1, SCATTER_AT)])
        (dh,), (pg1, od1) = k_back(6, dgate, dup, wg1, wu1, h1, dy, [Scatter(tg1, SCATTER_AT), Cross(pd1, CROSS_AT)])
        (dgate, dup, td0), (pu1, og1) = k_low(7, dh, wd0, gate, up, hidden, [Scatter(tu1, (0, 0.1, 1, 6, 14, 16, 16)), Cross(pg1, (0, 10))])
        (tg0, tu0), (pd0, ou1) = k_wide(8, a0, dgate, dup, [Scatter(td0, SCATTER_AT), Cross(pu1, CROSS_AT)])
        last = [
            Cross(pd0, CROSS_AT),
            Scatter(tg0, (0, 0.1, 1, 3, 7, 8.25, 8.7), True),
            Scatter(tu0, (1.2, 4, 4.1, 8, 8.2, 8.4, 8.8), True, (0, 2)),
            Scatter(tu0, (2, 5, 8.05, 8.1, 8.3, 8.5, 8.9), True, (1, 2)),
        ]
        (dx,), (od0, og0, *ou0) = k_back(9, dgate, dup, wg0, wu0, x, dh, last)
        ou0 = jnp.concatenate(ou0, 1)
        return dx[None], jnp.stack([og0, og1]), jnp.stack([ou0, ou1]), jnp.stack([od0, od1])

    states, cut = P(("rep", "r", "s"), None, None), P(None, "s", None)
    return jax.shard_map(
        step,
        mesh=mesh,
        in_specs=(states, states) + (cut,) * 3,
        out_specs=(states,) + (P("rep", "s", None),) * 3,
        check_vma=False,
    )
```
